16 devices in a mesh: dp: 2 (over y, z), cp: 8 (over x, core).
Axes of the slice: x: 4, y: 2, z: 1, core: 2. Of those that a mesh axis runs over, the one named last changes fastest.
The devices are a block of a 4x4x8 slice.
Arguments:
- vis_feat: bfloat16 [16, 4096, 1152], P(('dp', 'cp')), parts along dimension 0
- text_emb: bfloat16 [8192, 2304], P(('dp', 'cp')), parts along dimension 0
- img_pos: int32 [16], P('dp'), parts along dimension 0
- grad_y: bfloat16 [8192, 2304], P(('dp', 'cp')), parts along dimension 0
- pn_gain: bfloat16 [1152], replicated
- w_proj: bfloat16 [1152, 2304], replicated
- pre_gain: bfloat16 [2304], replicated
- w_query: bfloat16 [2304, 2048], replicated
- w_key: bfloat16 [2304, 1024], replicated
- w_value: bfloat16 [2304, 1024], replicated
- q_gain: bfloat16 [256], replicated
- k_gain: bfloat16 [256], replicated
- w_out: bfloat16 [2048, 2304], replicated
- post_gain: bfloat16 [2304], replicated
Outputs:
- output 1: bfloat16 [8192, 2304], P(('dp', 'cp')), parts along dimension 0
- output 2: bfloat16 [8192, 2304], P(('dp', 'cp')), parts along dimension 0
- output 3: bfloat16 [16, 4096, 1152], P(('dp', 'cp')), parts along dimension 0
- output 4: bfloat16 [2304], P('dp'), parts along dimension 0
- output 5: bfloat16 [2304, 2304], P('dp'), parts along dimension 0
- output 6: bfloat16 [4608], P('dp'), parts along dimension 0
- output 7: bfloat16 [4608, 2048], P('dp'), parts along dimension 0
- output 8: bfloat16 [4608, 1024], P('dp'), parts along dimension 0
- output 9: bfloat16 [4608, 1024], P('dp'), parts along dimension 0
- output 10: bfloat16 [512], P('dp'), parts along dimension 0
- output 11: bfloat16 [512], P('dp'), parts along dimension 0
- output 12: bfloat16 [4096, 2304], P('dp'), parts along dimension 0
- output 13: bfloat16 [4608], P('dp'), parts along dimension 0
There are 2 independent parts. The reference program is written for one: setup_inputs(seed, part) draws one part's arguments, and reference() takes and returns one part's arrays. A program takes and returns all parts, laid end to end along the dimension named above; an argument that names none is the same for every part.
All inputs are finite; a program needn't handle non-finite values.
Results may differ from the reference program's by a relative error of at most 0.02.
Values are sent between devices in bfloat16 or wider.
A program may use at most 768 MiB of HBM per device.

```python
import functools
import jax
import jax.numpy as jnp
from jax import lax

D = 2304
HEADS = 8
KV_HEADS = 4
HEAD = 256
DV = 1152
SEQ_DEV = 512
IMG_DEV = 1
GROUP = 8
GRID = 64
POOL = 4
SEQ = SEQ_DEV * GROUP
N_IMG = IMG_DEV * GROUP
SIDE = GRID // POOL
BLOCK = SIDE * SIDE
EPS = 1e-6
ROPE_BASE = 1000000.0
ROPE_SCALE = 8.0
NEG_BIG = -1e30


def place_images(rng_key):
    gap_key, perm_key = jax.random.split(rng_key)
    first_start = SEQ_DEV - BLOCK // 2
    spare = SEQ - N_IMG * BLOCK - first_start
    raw_gap = jax.random.randint(gap_key, (N_IMG,), 0, 8)
    weight = raw_gap * raw_gap * raw_gap
    gap_total = jnp.maximum(jnp.sum(weight), 1)
    gap_rows = spare * weight // gap_total
    slot_start = first_start + jnp.arange(N_IMG) * BLOCK + jnp.cumsum(gap_rows) - gap_rows
    slot_order = jax.random.permutation(perm_key, N_IMG)
    return slot_start[slot_order].astype(jnp.int32)


def draw_normal(rng_key, arr_shape, std_scale):
    return (jax.random.normal(rng_key, arr_shape, jnp.float32) * std_scale).astype(jnp.bfloat16)


def setup_inputs(seed: int = 0, part: int = 0) -> dict:
    base_key = jax.random.key(seed)
    part_keys = jax.random.split(jax.random.fold_in(base_key, part), 4)
    weight_keys = jax.random.split(jax.random.key(seed + 1), 10)
    return {
        'vis_feat': draw_normal(part_keys[0], (N_IMG, GRID * GRID, DV), 1.0),
        'text_emb': draw_normal(part_keys[1], (SEQ, D), 1.0),
        'img_pos': place_images(part_keys[2]),
        'grad_y': draw_normal(part_keys[3], (SEQ, D), 1.0),
        'pn_gain': draw_normal(weight_keys[0], (DV,), 0.3),
        'w_proj': draw_normal(weight_keys[1], (DV, D), DV ** -0.5),
        'pre_gain': draw_normal(weight_keys[2], (D,), 0.3),
        'w_query': draw_normal(weight_keys[3], (D, HEADS * HEAD), D ** -0.5),
        'w_key': draw_normal(weight_keys[4], (D, KV_HEADS * HEAD), D ** -0.5),
        'w_value': draw_normal(weight_keys[5], (D, KV_HEADS * HEAD), D ** -0.5),
        'q_gain': draw_normal(weight_keys[6], (HEAD,), 0.3),
        'k_gain': draw_normal(weight_keys[7], (HEAD,), 0.3),
        'w_out': draw_normal(weight_keys[8], (HEADS * HEAD, D), (HEADS * HEAD) ** -0.5),
        'post_gain': draw_normal(weight_keys[9], (D,), 0.3),
    }


def rms_scale(values, gain_vec):
    wide_vals = values.astype(jnp.float32)
    mean_sq = jnp.mean(wide_vals * wide_vals, axis=-1, keepdims=True)
    return wide_vals * lax.rsqrt(mean_sq + EPS) * (1.0 + gain_vec.astype(jnp.float32))


def rope_tables(positions):
    inv_freq = ROPE_BASE ** (-jnp.arange(0, HEAD, 2).astype(jnp.float32) / HEAD)
    rot_angle = (positions.astype(jnp.float32) / ROPE_SCALE)[:, None] * inv_freq[None, :]
    rot_angle = jnp.concatenate([rot_angle, rot_angle], axis=-1)
    return jnp.cos(rot_angle)[:, None, :], jnp.sin(rot_angle)[:, None, :]


def apply_rope(values, cos_t, sin_t):
    half_dim = values.shape[-1] // 2
    rotated = jnp.concatenate([-values[..., half_dim:], values[..., :half_dim]], axis=-1)
    return values * cos_t + rotated * sin_t


def project(vis_feat, pn_gain, w_proj):
    img_count = vis_feat.shape[0]
    patch_grid = vis_feat.reshape(img_count, SIDE, POOL, SIDE, POOL, DV).astype(jnp.float32)
    pooled = (jnp.sum(patch_grid, axis=(2, 4)) / (POOL * POOL)).astype(jnp.bfloat16)
    normed = rms_scale(pooled.reshape(img_count * BLOCK, DV), pn_gain).astype(jnp.bfloat16)
    return jnp.dot(normed, w_proj, preferred_element_type=jnp.float32).astype(jnp.bfloat16)


def attend_block(q_blk, start_blk, blk_index, k_heads, v_heads):
    groups = HEADS // KV_HEADS
    q_pos = blk_index * SEQ_DEV + jnp.arange(SEQ_DEV)
    key_pos = jnp.arange(SEQ)
    in_image = (start_blk[:, None] >= 0) & (key_pos[None, :] >= start_blk[:, None]) & (key_pos[None, :] < start_blk[:, None] + BLOCK)
    visible = (key_pos[None, :] <= q_pos[:, None]) | in_image
    q_grp = q_blk.reshape(SEQ_DEV, KV_HEADS, groups, HEAD).astype(jnp.float32)
    scores = jnp.einsum('qkgd,skd->kgqs', q_grp, k_heads.astype(jnp.float32)) * HEAD ** -0.5
    scores = jnp.where(visible[None, None], scores, NEG_BIG)
    prob_lo = jax.nn.softmax(scores, axis=-1).astype(jnp.bfloat16)
    attn_blk = jnp.einsum('kgqs,skd->qkgd', prob_lo.astype(jnp.float32), v_heads.astype(jnp.float32))
    return attn_blk.astype(jnp.bfloat16).reshape(SEQ_DEV, HEADS * HEAD)


def forward(vis_feat, text_emb, pn_gain, w_proj, pre_gain, w_query, w_key, w_value, q_gain, k_gain, w_out, post_gain, img_pos):
    soft_tok = project(vis_feat, pn_gain, w_proj)
    img_rows = (img_pos[:, None] + jnp.arange(BLOCK)[None, :]).reshape(-1)
    merged = text_emb.at[img_rows].set(soft_tok)
    starts = jnp.full((SEQ,), -1, jnp.int32).at[img_rows].set(jnp.repeat(img_pos, BLOCK))
    hidden = rms_scale(merged, pre_gain).astype(jnp.bfloat16)
    q_raw = jnp.dot(hidden, w_query, preferred_element_type=jnp.float32).astype(jnp.bfloat16).reshape(SEQ, HEADS, HEAD)
    k_raw = jnp.dot(hidden, w_key, preferred_element_type=jnp.float32).astype(jnp.bfloat16).reshape(SEQ, KV_HEADS, HEAD)
    v_heads = jnp.dot(hidden, w_value, preferred_element_type=jnp.float32).astype(jnp.bfloat16).reshape(SEQ, KV_HEADS, HEAD)
    cos_t, sin_t = rope_tables(jnp.arange(SEQ))
    q_heads = apply_rope(rms_scale(q_raw, q_gain), cos_t, sin_t).astype(jnp.bfloat16)
    k_heads = apply_rope(rms_scale(k_raw, k_gain), cos_t, sin_t).astype(jnp.bfloat16)
    block_fn = jax.checkpoint(attend_block)
    attn_out = lax.map(lambda blk_args: block_fn(blk_args[0], blk_args[1], blk_args[2], k_heads, v_heads), (q_heads.reshape(GROUP, SEQ_DEV, HEADS, HEAD), starts.reshape(GROUP, SEQ_DEV), jnp.arange(GROUP)))
    attn_out = attn_out.reshape(SEQ, HEADS * HEAD)
    proj_out = jnp.dot(attn_out, w_out, preferred_element_type=jnp.float32).astype(jnp.bfloat16)
    return (merged.astype(jnp.float32) + rms_scale(proj_out, post_gain)).astype(jnp.bfloat16)


def reference(vis_feat, text_emb, img_pos, grad_y, pn_gain, w_proj, pre_gain, w_query, w_key, w_value, q_gain, k_gain, w_out, post_gain):
    y_out, pullback = jax.vjp(functools.partial(forward, img_pos=img_pos), vis_feat, text_emb, pn_gain, w_proj, pre_gain, w_query, w_key, w_value, q_gain, k_gain, w_out, post_gain)
    grad_list = pullback(grad_y)
    return (y_out, grad_list[1], grad_list[0], grad_list[2], grad_list[3], grad_list[4], grad_list[5], grad_list[6], grad_list[7], grad_list[8], grad_list[9], grad_list[10], grad_list[11])
```

```python
import functools
import jax
import jax.numpy as jnp
from jax import lax
from jax.experimental import pallas as pl
from jax.experimental.pallas import tpu as pltpu
from jax.sharding import PartitionSpec as P

GRID = 64
POOL = 4
EPS = 1e-6
ROPE_BASE = 1000000.0
ROPE_SCALE = 8.0
NEG_BIG = -1e30
BF = jnp.bfloat16
F32 = jnp.float32


def rms_scale(values, gain_vec):
    wide_vals = values.astype(F32)
    mean_sq = jnp.mean(wide_vals * wide_vals, axis=-1, keepdims=True)
    return wide_vals * lax.rsqrt(mean_sq + EPS) * (1.0 + gain_vec)


def gain_norm(values, gain_vec):
    return rms_scale(values, gain_vec).astype(BF)


def rope_tables(positions, head_dim):
    inv_freq = ROPE_BASE ** (-jnp.arange(0, head_dim, 2).astype(F32) / head_dim)
    rot_angle = (positions.astype(F32) / ROPE_SCALE)[:, None] * inv_freq[None, :]
    rot_angle = jnp.concatenate([rot_angle, rot_angle], axis=-1)
    return jnp.cos(rot_angle), jnp.sin(rot_angle)


def apply_rope(values, cos_t, sin_t):
    half_dim = values.shape[-1] // 2
    rotated = jnp.concatenate([-values[..., half_dim:], values[..., :half_dim]], axis=-1)
    return values * cos_t + rotated * sin_t


def head_rotate(raw, gain, cos_t, sin_t):
    return apply_rope(rms_scale(raw, gain), cos_t, sin_t).astype(BF)


def post_residual(merged, proj_out, gain_vec):
    return (merged.astype(F32) + rms_scale(proj_out, gain_vec)).astype(BF)


def mm(a, b, dims=((1,), (0,))):
    return lax.dot_general(a, b, (dims, ((), ())), preferred_element_type=F32)


def attn_fwd_body(lmax_ref, lim_ref, q_ref, k_ref, vt_ref, o_ref, of_ref, lse_ref, acc_ref, m_ref, l_ref, *, bq, bo):
    qi = pl.program_id(0)
    q0 = qi * bq
    acc_ref[...] = jnp.zeros_like(acc_ref)
    m_ref[...] = jnp.full_like(m_ref, NEG_BIG)
    l_ref[...] = jnp.zeros_like(l_ref)
    q = q_ref[...]

    def tile(k0, bk, masked):
        s = mm(k_ref[pl.ds(k0, bk), :], q, ((1,), (1,)))
        if masked:
            kpos = k0 + lax.broadcasted_iota(jnp.int32, s.shape, 0)
            s = jnp.where(kpos <= lim_ref[0], s, NEG_BIG)
        m_old = m_ref[...]
        m_new = jnp.maximum(m_old, jnp.max(s, axis=0, keepdims=True))
        p = jnp.exp(s - m_new)
        alpha = jnp.exp(m_old - m_new)
        m_ref[...] = m_new
        l_ref[...] = l_ref[...] * alpha + jnp.sum(p, axis=0, keepdims=True)
        acc_ref[...] = acc_ref[...] * alpha + mm(vt_ref[:, pl.ds(k0, bk)], p.astype(BF))

    def step(kb, carry):
        tile(pl.multiple_of(kb * bq, bq), bq, False)
        return carry

    lax.fori_loop(0, qi, step, 0)
    tile(pl.multiple_of(q0, bq), bq, True)

    @pl.when(lmax_ref[qi] >= q0 + bq)
    def _():
        tile(pl.multiple_of(q0 + bq, bq), bo, True)

    l = l_ref[...]
    o = jnp.transpose(acc_ref[...] / l)
    of_ref[...] = o
    o_ref[...] = o.astype(BF)
    lse_ref[0] = m_ref[...] + jnp.log(l)


def attn_fwd(q, k, vt, lim, lmax, bq, bo):
    seq, hd = q.shape
    nq = seq // bq
    body = functools.partial(attn_fwd_body, bq=bq, bo=bo)
    row = pl.BlockSpec((1, 1, bq), lambda i, s: (i, 0, 0))
    tile = pl.BlockSpec((bq, hd), lambda i, s: (i, 0))
    return pl.pallas_call(
        body,
        out_shape=(jax.ShapeDtypeStruct((seq, hd), BF), jax.ShapeDtypeStruct((seq, hd), F32), jax.ShapeDtypeStruct((nq, 1, bq), F32)),
        grid_spec=pltpu.PrefetchScalarGridSpec(
            num_scalar_prefetch=1,
            grid=(nq,),
            in_specs=[row, tile, pl.BlockSpec((seq, hd), lambda i, s: (0, 0)), pl.BlockSpec((hd, seq), lambda i, s: (0, 0))],
            out_specs=(tile, tile, row),
            scratch_shapes=[pltpu.VMEM((hd, bq), F32), pltpu.VMEM((1, bq), F32), pltpu.VMEM((1, bq), F32)],
        ),
        compiler_params=pltpu.CompilerParams(dimension_semantics=('arbitrary',), vmem_limit_bytes=48 * 1024 * 1024),
        cost_estimate=pl.CostEstimate(flops=2 * seq * seq * hd, bytes_accessed=seq * hd * 14, transcendentals=seq * seq // 2),
        name='attn_fwd',
    )(lmax, lim, q, k, vt)


def attn_bwd_body(lmax_ref, lim_ref, lse_ref, dl_ref, q_ref, do_ref, k_ref, kt_ref, v_ref, dq_ref, dk_ref, dv_ref, acc_ref, *, bq, bo, scale):
    qi = pl.program_id(0)
    q0 = qi * bq

    @pl.when(qi == 0)
    def _():
        dk_ref[...] = jnp.zeros_like(dk_ref)
        dv_ref[...] = jnp.zeros_like(dv_ref)

    acc_ref[...] = jnp.zeros_like(acc_ref)
    q = q_ref[...]
    do = do_ref[...]
    lse = lse_ref[0]
    delta = dl_ref[0]

    def tile(k0, bk, masked):
        ks = pl.ds(k0, bk)
        s = mm(k_ref[ks, :], q, ((1,), (1,)))
        if masked:
            kpos = k0 + lax.broadcasted_iota(jnp.int32, s.shape, 0)
            s = jnp.where(kpos <= lim_ref[0], s, NEG_BIG)
        p = jnp.exp(s - lse)
        dp = mm(v_ref[ks, :], do, ((1,), (1,)))
        dv_ref[ks, :] += mm(p.astype(BF), do)
        ds = (p * (dp - delta)).astype(BF)
        dk_ref[ks, :] += mm(ds, q)
        acc_ref[...] += mm(kt_ref[:, ks], ds)

    def step(kb, carry):
        tile(pl.multiple_of(kb * bq, bq), bq, False)
        return carry

    lax.fori_loop(0, qi, step, 0)
    tile(pl.multiple_of(q0, bq), bq, True)

    @pl.when(lmax_ref[qi] >= q0 + bq)
    def _():
        tile(pl.multiple_of(q0 + bq, bq), bo, True)

    dq_ref[...] = (jnp.transpose(acc_ref[...]) * scale).astype(BF)


def attn_bwd(q, k, kt, v, do, lse, delta, lim, lmax, bq, bo, scale):
    seq, hd = q.shape
    nq = seq // bq
    body = functools.partial(attn_bwd_body, bq=bq, bo=bo, scale=scale)
    row = pl.BlockSpec((1, 1, bq), lambda i, s: (i, 0, 0))
    tile = pl.BlockSpec((bq, hd), lambda i, s: (i, 0))
    whole = pl.BlockSpec((seq, hd), lambda i, s: (0, 0))
    return pl.pallas_call(
        body,
        out_shape=(jax.ShapeDtypeStruct((seq, hd), BF), jax.ShapeDtypeStruct((seq, hd), F32), jax.ShapeDtypeStruct((seq, hd), F32)),
        grid_spec=pltpu.PrefetchScalarGridSpec(
            num_scalar_prefetch=1,
            grid=(nq,),
            in_specs=[row, row, row, tile, tile, whole, pl.BlockSpec((hd, seq), lambda i, s: (0, 0)), whole],
            out_specs=(tile, whole, whole),
            scratch_shapes=[pltpu.VMEM((hd, bq), F32)],
        ),
        compiler_params=pltpu.CompilerParams(dimension_semantics=('arbitrary',), vmem_limit_bytes=56 * 1024 * 1024),
        cost_estimate=pl.CostEstimate(flops=5 * seq * seq * hd, bytes_accessed=seq * hd * 20, transcendentals=seq * seq // 2),
        name='attn_bwd',
    )(lmax, lim, lse, delta, q, do, k, kt, v)


def solution(mesh):
    size = mesh.shape['cp']
    seq_spec = P(('dp', 'cp'))
    part_spec = P('dp')
    rep_spec = P()

    def device_body(vis_loc, text_loc, img_pos, grad_y, pn_gain, w_proj, pre_gain, w_query, w_key, w_value, q_gain, k_gain, w_out, post_gain):
        rank = lax.axis_index('cp')
        even = rank % 2 == 0
        loc, dim = text_loc.shape
        seq = loc * size
        dim_v = vis_loc.shape[2]
        hd = q_gain.shape[0]
        heads = w_query.shape[1] // hd
        kv_heads = w_key.shape[1] // hd
        side = GRID // POOL
        block = side * side
        n_img = img_pos.shape[0]
        scale = hd ** -0.5
        bq = min(512, seq // 2)
        nq = seq // bq
        pn_f, pre_f, qg_f, kg_f, post_f = (g.astype(F32) for g in (pn_gain, pre_gain, q_gain, k_gain, post_gain))

        patch = jnp.arange(GRID * GRID)
        cell = (patch // (GRID * POOL)) * side + (patch % GRID) // POOL
        pool_mat = (jnp.arange(block)[:, None] == cell[None, :]).astype(BF)
        pooled = (mm(pool_mat, vis_loc[0]) / (POOL * POOL)).astype(BF)
        pooled_all = lax.all_gather(pooled, 'cp', tiled=True)

        pos_all = jnp.arange(seq)
        off_all = pos_all[:, None] - img_pos[None, :]
        in_all = (off_all >= 0) & (off_all < block)
        lim_all = jnp.where(jnp.any(in_all, axis=1), jnp.sum(jnp.where(in_all, img_pos[None, :] + block - 1, 0), axis=1), pos_all).astype(jnp.int32)
        lim = lim_all.reshape(nq, 1, bq)
        lmax = jnp.max(lim_all.reshape(nq, bq), axis=1)
        q_pos = rank * loc + jnp.arange(loc)
        offset = q_pos[:, None] - img_pos[None, :]
        in_blk = (offset >= 0) & (offset < block)
        is_img = jnp.any(in_blk, axis=1)
        flat_row = jnp.sum(jnp.where(in_blk, jnp.arange(n_img)[None, :] * block + offset, 0), axis=1)
        flat_row = jnp.where(is_img, flat_row, -1)
        img_mask = is_img[:, None]
        sel = (flat_row[:, None] == jnp.arange(n_img * block)[None, :]).astype(BF)

        pooled_rows = mm(sel, pooled_all).astype(BF)
        normed_rows, norm_pull = jax.vjp(gain_norm, pooled_rows, pn_f)
        soft_rows = mm(normed_rows, w_proj).astype(BF)
        merged = jnp.where(img_mask, soft_rows, text_loc)
        hidden, pre_pull = jax.vjp(gain_norm, merged, pre_f)
        hidden_all = lax.all_gather(hidden, 'cp', tiled=True)

        kv_id = rank * kv_heads // size
        wq_h = lax.dynamic_slice(w_query, (0, rank * hd), (dim, hd))
        wk_h = lax.dynamic_slice(w_key, (0, kv_id * hd), (dim, hd))
        wv_h = lax.dynamic_slice(w_value, (0, kv_id * hd), (dim, hd))
        wo_h = lax.dynamic_slice(w_out, (rank * hd, 0), (hd, dim))
        q_raw = mm(hidden_all, wq_h).astype(BF)
        k_raw = mm(hidden_all, wk_h).astype(BF)
        v = mm(hidden_all, wv_h).astype(BF)
        cos_t, sin_t = rope_tables(pos_all, hd)
        rot = functools.partial(head_rotate, cos_t=cos_t, sin_t=sin_t)
        q, q_pull = jax.vjp(rot, q_raw, qg_f)
        k, k_pull = jax.vjp(rot, k_raw, kg_f)
        qs = (q.astype(F32) * scale).astype(BF)

        o, o_wide, lse = attn_fwd(qs, k, v.T, lim, lmax, bq, block)
        o_rows = lax.all_to_all(o.reshape(size, loc, hd), 'cp', 0, 0, tiled=True)
        o_rows = o_rows.transpose(1, 0, 2).reshape(loc, heads * hd)
        proj_out = mm(o_rows, w_out).astype(BF)
        y_loc, post_pull = jax.vjp(post_residual, merged, proj_out, post_f)
        d_resid, d_proj, g_post = post_pull(grad_y)

        d_proj_all = lax.all_gather(d_proj, 'cp', tiled=True)
        d_o = mm(d_proj_all, wo_h, ((1,), (1,))).astype(BF)
        g_out_h = mm(o, d_proj_all, ((0,), (0,))).astype(BF)
        g_out = lax.all_gather(g_out_h, 'cp', tiled=True)
        delta = jnp.sum(d_o.astype(F32) * o_wide, axis=1).reshape(nq, 1, bq)
        d_q, d_k_part, d_v_part = attn_bwd(qs, k, k.T, v, d_o, lse, delta, lim, lmax, bq, block, scale)
        swap = [(i, i ^ 1) for i in range(size)]
        got = lax.ppermute(jnp.where(even, d_v_part, d_k_part), 'cp', swap)
        d_kv = (jnp.where(even, d_k_part, d_v_part) + got).astype(BF)
        d_q_raw, g_q_gain = q_pull(d_q)
        d_k_raw, g_k_gain = k_pull(d_kv)
        g_k_gain = jnp.where(even, g_k_gain, 0.0)
        d_head = jnp.concatenate([d_q_raw, jnp.where(even, d_k_raw, d_kv)], axis=1)
        d_rows = lax.all_to_all(d_head.reshape(size, loc, 2 * hd), 'cp', 0, 0, tiled=True)
        g_head = mm(hidden_all, d_head, ((0,), (0,))).astype(BF)
        g_head_all = lax.all_gather(g_head, 'cp')
        g_query = g_head_all[:, :, :hd].transpose(1, 0, 2).reshape(dim, heads * hd)
        g_key = g_head_all[0::2, :, hd:].transpose(1, 0, 2).reshape(dim, kv_heads * hd)
        g_value = g_head_all[1::2, :, hd:].transpose(1, 0, 2).reshape(dim, kv_heads * hd)

        d_q_flat = d_rows[:, :, :hd].transpose(1, 0, 2).reshape(loc, heads * hd)
        d_k_flat = d_rows[0::2, :, hd:].transpose(1, 0, 2).reshape(loc, kv_heads * hd)
        d_v_flat = d_rows[1::2, :, hd:].transpose(1, 0, 2).reshape(loc, kv_heads * hd)
        nt = ((1,), (1,))
        d_hidden = (mm(d_q_flat, w_query, nt) + mm(d_k_flat, w_key, nt) + mm(d_v_flat, w_value, nt)).astype(BF)
        d_merged_attn, g_pre = pre_pull(d_hidden)
        d_merged = (d_resid.astype(F32) + d_merged_attn.astype(F32)).astype(BF)
        zero = jnp.zeros((), BF)
        grad_text = jnp.where(img_mask, zero, d_merged)
        d_soft = jnp.where(img_mask, d_merged, zero)
        d_normed = mm(d_soft, w_proj, nt).astype(BF)
        d_pooled_rows, g_pn = norm_pull(d_normed)
        d_pooled_all = mm(sel, d_pooled_rows, ((0,), (0,))).astype(BF)
        d_pooled = lax.psum_scatter(d_pooled_all, 'cp', scatter_dimension=0, tiled=True)
        spread = (d_pooled.astype(F32) / (POOL * POOL)).astype(BF)
        grad_vis = mm(pool_mat, spread, ((0,), (0,))).astype(BF)[None]

        g_proj_part = mm(normed_rows, d_soft, ((0,), (0,)))
        g_proj_loc = lax.psum_scatter(g_proj_part, 'cp', scatter_dimension=0, tiled=True).astype(BF)
        g_proj = lax.all_gather(g_proj_loc, 'cp', tiled=True)
        small = lax.psum(jnp.concatenate([g_pn, g_pre, g_q_gain, g_k_gain, g_post]), 'cp').astype(BF)
        edges = [0, dim_v, dim_v + dim, dim_v + dim + hd, dim_v + dim + 2 * hd, dim_v + 2 * dim + 2 * hd]
        s_pn, s_pre, s_q, s_k, s_post = (small[a:b] for a, b in zip(edges[:-1], edges[1:]))
        return y_loc, grad_text, grad_vis, s_pn, g_proj, s_pre, g_query, g_key, g_value, s_q, s_k, g_out, s_post

    in_specs = (seq_spec, seq_spec, part_spec, seq_spec) + (rep_spec,) * 10
    out_specs = (seq_spec, seq_spec, seq_spec) + (part_spec,) * 10
    return jax.shard_map(device_body, mesh=mesh, in_specs=in_specs, out_specs=out_specs, check_vma=False)
```

```python
import functools
import jax
import jax.numpy as jnp
from jax import lax
from jax.experimental import pallas as pl
from jax.experimental.pallas import tpu as pltpu
from jax.sharding import PartitionSpec as P

GRID = 64
POOL = 4
EPS = 1e-6
ROPE_BASE = 1000000.0
ROPE_SCALE = 8.0
NEG_BIG = -1e30
BF = jnp.bfloat16
F32 = jnp.float32


def rms_scale(values, gain_vec):
    wide_vals = values.astype(F32)
    mean_sq = jnp.mean(wide_vals * wide_vals, axis=-1, keepdims=True)
    return wide_vals * lax.rsqrt(mean_sq + EPS) * (1.0 + gain_vec)


def gain_norm(values, gain_vec):
    return rms_scale(values, gain_vec).astype(BF)


def rope_tables(positions, head_dim):
    inv_freq = ROPE_BASE ** (-jnp.arange(0, head_dim, 2).astype(F32) / head_dim)
    rot_angle = (positions.astype(F32) / ROPE_SCALE)[:, None] * inv_freq[None, :]
    return jnp.cos(rot_angle), jnp.sin(rot_angle)


def post_residual(merged, proj_out, gain_vec):
    return (merged.astype(F32) + rms_scale(proj_out, gain_vec)).astype(BF)


def mm(a, b, dims=((1,), (0,))):
    return lax.dot_general(a, b, (dims, ((), ())), preferred_element_type=F32)


def attn_fwd_body(lmax_ref, lim_ref, q_ref, k_ref, vt_ref, o_ref, of_ref, lse_ref, acc_ref, m_ref, l_ref, *, bq, bo):
    qi = pl.program_id(0)
    q0 = qi * bq
    acc_ref[...] = jnp.zeros_like(acc_ref)
    m_ref[...] = jnp.full_like(m_ref, NEG_BIG)
    l_ref[...] = jnp.zeros_like(l_ref)
    q = q_ref[...]

    def tile(k0, bk, masked):
        s = mm(k_ref[pl.ds(k0, bk), :], q, ((1,), (1,)))
        if masked:
            kpos = k0 + lax.broadcasted_iota(jnp.int32, s.shape, 0)
            s = jnp.where(kpos <= lim_ref[0], s, NEG_BIG)
        m_old = m_ref[...]
        m_new = jnp.maximum(m_old, jnp.max(s, axis=0, keepdims=True))
        p = jnp.exp(s - m_new)
        alpha = jnp.exp(m_old - m_new)
        m_ref[...] = m_new
        l_ref[...] = l_ref[...] * alpha + jnp.sum(p, axis=0, keepdims=True)
        acc_ref[...] = acc_ref[...] * alpha + mm(vt_ref[:, pl.ds(k0, bk)], p.astype(BF))

    def step(kb, carry):
        tile(pl.multiple_of(kb * bq, bq), bq, False)
        return carry

    lax.fori_loop(0, qi, step, 0)
    tile(pl.multiple_of(q0, bq), bq, True)

    @pl.when(lmax_ref[qi] >= q0 + bq)
    def _():
        tile(pl.multiple_of(q0 + bq, bq), bo, True)

    l = l_ref[...]
    o = jnp.transpose(acc_ref[...] / l)
    of_ref[...] = o
    o_ref[...] = o.astype(BF)
    lse_ref[0] = m_ref[...] + jnp.log(l)


def attn_fwd(q, k, vt, lim, lmax, bq, bo):
    seq, hd = q.shape
    nq = seq // bq
    body = functools.partial(attn_fwd_body, bq=bq, bo=bo)
    row = pl.BlockSpec((1, 1, bq), lambda i, s: (i, 0, 0))
    tile = pl.BlockSpec((bq, hd), lambda i, s: (i, 0))
    return pl.pallas_call(
        body,
        out_shape=(jax.ShapeDtypeStruct((seq, hd), BF), jax.ShapeDtypeStruct((seq, hd), F32), jax.ShapeDtypeStruct((nq, 1, bq), F32)),
        grid_spec=pltpu.PrefetchScalarGridSpec(
            num_scalar_prefetch=1,
            grid=(nq,),
            in_specs=[row, tile, pl.BlockSpec((seq, hd), lambda i, s: (0, 0)), pl.BlockSpec((hd, seq), lambda i, s: (0, 0))],
            out_specs=(tile, tile, row),
            scratch_shapes=[pltpu.VMEM((hd, bq), F32), pltpu.VMEM((1, bq), F32), pltpu.VMEM((1, bq), F32)],
        ),
        compiler_params=pltpu.CompilerParams(dimension_semantics=('arbitrary',), vmem_limit_bytes=48 * 1024 * 1024),
        cost_estimate=pl.CostEstimate(flops=2 * seq * seq * hd, bytes_accessed=seq * hd * 14, transcendentals=seq * seq // 2),
        name='attn_fwd',
    )(lmax, lim, q, k, vt)


def attn_bwd_body(lmax_ref, even_ref, lim_ref, lse_ref, dl_ref, q_ref, do_ref, k_ref, kt_ref, v_ref, dq_ref, keep_ref, send_ref, acc_ref, dk_ref, dv_ref, *, bq, bo, scale):
    qi = pl.program_id(0)
    q0 = qi * bq

    @pl.when(qi == 0)
    def _():
        dk_ref[...] = jnp.zeros_like(dk_ref)
        dv_ref[...] = jnp.zeros_like(dv_ref)

    acc_ref[...] = jnp.zeros_like(acc_ref)
    q = q_ref[...]
    do = do_ref[...]
    lse = lse_ref[0]
    delta = dl_ref[0]

    def tile(k0, bk, masked):
        ks = pl.ds(k0, bk)
        s = mm(k_ref[ks, :], q, ((1,), (1,)))
        if masked:
            kpos = k0 + lax.broadcasted_iota(jnp.int32, s.shape, 0)
            s = jnp.where(kpos <= lim_ref[0], s, NEG_BIG)
        p = jnp.exp(s - lse)
        dp = mm(v_ref[ks, :], do, ((1,), (1,)))
        dv_ref[ks, :] += mm(p.astype(BF), do)
        ds = (p * (dp - delta)).astype(BF)
        dk_ref[ks, :] += mm(ds, q)
        acc_ref[...] += mm(kt_ref[:, ks], ds)

    def step(kb, carry):
        tile(pl.multiple_of(kb * bq, bq), bq, False)
        return carry

    lax.fori_loop(0, qi, step, 0)
    tile(pl.multiple_of(q0, bq), bq, True)

    @pl.when(lmax_ref[qi] >= q0 + bq)
    def _():
        tile(pl.multiple_of(q0 + bq, bq), bo, True)

    dq_ref[...] = (jnp.transpose(acc_ref[...]) * scale).astype(BF)
    last = qi == pl.num_programs(0) - 1

    @pl.when(last & (even_ref[0] == 1))
    def _():
        keep_ref[...] = dk_ref[...]
        send_ref[...] = dv_ref[...]

    @pl.when(last & (even_ref[0] == 0))
    def _():
        keep_ref[...] = dv_ref[...]
        send_ref[...] = dk_ref[...]


def attn_bwd(q, k, kt, v, do, lse, delta, lim, lmax, even, bq, bo, scale):
    seq, hd = q.shape
    nq = seq // bq
    body = functools.partial(attn_bwd_body, bq=bq, bo=bo, scale=scale)
    row = pl.BlockSpec((1, 1, bq), lambda i, s, e: (i, 0, 0))
    tile = pl.BlockSpec((bq, hd), lambda i, s, e: (i, 0))
    whole = pl.BlockSpec((seq, hd), lambda i, s, e: (0, 0))
    return pl.pallas_call(
        body,
        out_shape=(jax.ShapeDtypeStruct((seq, hd), BF), jax.ShapeDtypeStruct((seq, hd), F32), jax.ShapeDtypeStruct((seq, hd), F32)),
        grid_spec=pltpu.PrefetchScalarGridSpec(
            num_scalar_prefetch=2,
            grid=(nq,),
            in_specs=[row, row, row, tile, tile, whole, pl.BlockSpec((hd, seq), lambda i, s, e: (0, 0)), whole],
            out_specs=(tile, whole, whole),
            scratch_shapes=[pltpu.VMEM((hd, bq), F32), pltpu.VMEM((seq, hd), F32), pltpu.VMEM((seq, hd), F32)],
        ),
        compiler_params=pltpu.CompilerParams(dimension_semantics=('arbitrary',), vmem_limit_bytes=56 * 1024 * 1024),
        cost_estimate=pl.CostEstimate(flops=5 * seq * seq * hd, bytes_accessed=seq * hd * 20, transcendentals=seq * seq // 2),
        name='attn_bwd',
    )(lmax, even, lim, lse, delta, q, do, k, kt, v)


def turn(y, cos_t, sin_t):
    half = y.shape[1] // 2
    lo, hi = y[:, :half], y[:, half:]
    return jnp.concatenate([lo * cos_t - hi * sin_t, hi * cos_t + lo * sin_t], axis=1)


def turn_back(d, cos_t, sin_t):
    half = d.shape[1] // 2
    lo, hi = d[:, :half], d[:, half:]
    return jnp.concatenate([lo * cos_t + hi * sin_t, hi * cos_t - lo * sin_t], axis=1)


def qkv_body(h_ref, w_ref, cos_ref, sin_ref, qg_ref, kg_ref, qr_ref, kr_ref, q_ref, k_ref, kt_ref, v_ref, vt_ref, *, hd, scale):
    acc = mm(h_ref[...], w_ref[...])
    cos_t, sin_t = cos_ref[...], sin_ref[...]
    q_raw = acc[:, :hd].astype(BF)
    k_raw = acc[:, hd:2 * hd].astype(BF)
    v = acc[:, 2 * hd:].astype(BF)
    qr_ref[...] = q_raw
    kr_ref[...] = k_raw
    v_ref[...] = v
    vt_ref[...] = jnp.transpose(v.astype(F32)).astype(BF)
    q = turn(rms_scale(q_raw, qg_ref[...]), cos_t, sin_t).astype(BF)
    q_ref[...] = (q.astype(F32) * scale).astype(BF)
    k = turn(rms_scale(k_raw, kg_ref[...]), cos_t, sin_t).astype(BF)
    k_ref[...] = k
    kt_ref[...] = jnp.transpose(k.astype(F32)).astype(BF)


def qkv_call(h, w, cos_t, sin_t, qg, kg, bm, scale):
    seq, dim = h.shape
    hd = w.shape[1] // 3
    tile = pl.BlockSpec((bm, hd), lambda i: (i, 0))
    tall = pl.BlockSpec((hd, bm), lambda i: (0, i))
    table = pl.BlockSpec((bm, hd // 2), lambda i: (i, 0))
    gain = pl.BlockSpec((1, hd), lambda i: (0, 0))
    flat = jax.ShapeDtypeStruct((seq, hd), BF)
    high = jax.ShapeDtypeStruct((hd, seq), BF)
    return pl.pallas_call(
        functools.partial(qkv_body, hd=hd, scale=scale),
        out_shape=(flat, flat, flat, flat, high, flat, high),
        grid=(seq // bm,),
        in_specs=[pl.BlockSpec((bm, dim), lambda i: (i, 0)), pl.BlockSpec((dim, 3 * hd), lambda i: (0, 0)), table, table, gain, gain],
        out_specs=(tile, tile, tile, tile, tall, tile, tall),
        compiler_params=pltpu.CompilerParams(dimension_semantics=('arbitrary',), vmem_limit_bytes=40 * 1024 * 1024),
        cost_estimate=pl.CostEstimate(flops=6 * seq * dim * hd, bytes_accessed=seq * dim * 2 + seq * hd * 18, transcendentals=0),
        name='qkv',
    )(h, w, cos_t, sin_t, qg, kg)


def norm_back(x_raw, dy, gain):
    x = x_raw.astype(F32)
    r = lax.rsqrt(jnp.mean(x * x, axis=-1, keepdims=True) + EPS)
    xr = x * r
    g_gain = jnp.sum(dy * xr, axis=0, keepdims=True)
    dx = dy * (1.0 + gain)
    return r * (dx - xr * jnp.mean(dx * xr, axis=-1, keepdims=True)), g_gain


def head_back_body(even_ref, dq_ref, keep_ref, got_ref, qr_ref, kr_ref, cos_ref, sin_ref, qg_ref, kg_ref, out_ref, gq_ref, gk_ref, *, hd):
    @pl.when(pl.program_id(0) == 0)
    def _():
        gq_ref[...] = jnp.zeros_like(gq_ref)
        gk_ref[...] = jnp.zeros_like(gk_ref)

    cos_t, sin_t = cos_ref[...], sin_ref[...]
    dq, gq = norm_back(qr_ref[...], turn_back(dq_ref[...].astype(F32), cos_t, sin_t), qg_ref[...])
    out_ref[:, :hd] = dq.astype(BF)
    gq_ref[...] += gq
    d_kv = (keep_ref[...] + got_ref[...]).astype(BF)

    @pl.when(even_ref[0] == 1)
    def _():
        dk, gk = norm_back(kr_ref[...], turn_back(d_kv.astype(F32), cos_t, sin_t), kg_ref[...])
        out_ref[:, hd:] = dk.astype(BF)
        gk_ref[...] += gk

    @pl.when(even_ref[0] == 0)
    def _():
        out_ref[:, hd:] = d_kv


def head_back(even, dq, keep, got, qr, kr, cos_t, sin_t, qg, kg, bm):
    seq, hd = dq.shape
    tile = pl.BlockSpec((bm, hd), lambda i, s: (i, 0))
    table = pl.BlockSpec((bm, hd // 2), lambda i, s: (i, 0))
    gain = pl.BlockSpec((1, hd), lambda i, s: (0, 0))
    vec = jax.ShapeDtypeStruct((1, hd), F32)
    return pl.pallas_call(
        functools.partial(head_back_body, hd=hd),
        out_shape=(jax.ShapeDtypeStruct((seq, 2 * hd), BF), vec, vec),
        grid_spec=pltpu.PrefetchScalarGridSpec(
            num_scalar_prefetch=1,
            grid=(seq // bm,),
            in_specs=[tile, tile, tile, tile, tile, table, table, gain, gain],
            out_specs=(pl.BlockSpec((bm, 2 * hd), lambda i, s: (i, 0)), gain, gain),
        ),
        compiler_params=pltpu.CompilerParams(dimension_semantics=('arbitrary',), vmem_limit_bytes=40 * 1024 * 1024),
        cost_estimate=pl.CostEstimate(flops=40 * seq * hd * 100, bytes_accessed=seq * hd * 22, transcendentals=0),
        name='head_back',
    )(even, dq, keep, got, qr, kr, cos_t, sin_t, qg, kg)


def solution(mesh):
    size = mesh.shape['cp']
    seq_spec = P(('dp', 'cp'))
    part_spec = P('dp')
    rep_spec = P()

    def device_body(vis_loc, text_loc, img_pos, grad_y, pn_gain, w_proj, pre_gain, w_query, w_key, w_value, q_gain, k_gain, w_out, post_gain):
        rank = lax.axis_index('cp')
        even = rank % 2 == 0
        loc, dim = text_loc.shape
        seq = loc * size
        dim_v = vis_loc.shape[2]
        hd = q_gain.shape[0]
        heads = w_query.shape[1] // hd
        kv_heads = w_key.shape[1] // hd
        side = GRID // POOL
        block = side * side
        n_img = img_pos.shape[0]
        scale = hd ** -0.5
        bq = min(512, seq // 2)
        nq = seq // bq
        pn_f, pre_f, qg_f, kg_f, post_f = (g.astype(F32) for g in (pn_gain, pre_gain, q_gain, k_gain, post_gain))

        patch = jnp.arange(GRID * GRID)
        cell = (patch // (GRID * POOL)) * side + (patch % GRID) // POOL
        pool_mat = (jnp.arange(block)[:, None] == cell[None, :]).astype(BF)
        pooled = (mm(pool_mat, vis_loc[0]) / (POOL * POOL)).astype(BF)
        pooled_all = lax.all_gather(pooled, 'cp', tiled=True)

        pos_all = jnp.arange(seq)
        off_all = pos_all[:, None] - img_pos[None, :]
        in_all = (off_all >= 0) & (off_all < block)
        lim_all = jnp.where(jnp.any(in_all, axis=1), jnp.sum(jnp.where(in_all, img_pos[None, :] + block - 1, 0), axis=1), pos_all).astype(jnp.int32)
        lim = lim_all.reshape(nq, 1, bq)
        lmax = jnp.max(lim_all.reshape(nq, bq), axis=1)
        q_pos = rank * loc + jnp.arange(loc)
        offset = q_pos[:, None] - img_pos[None, :]
        in_blk = (offset >= 0) & (offset < block)
        is_img = jnp.any(in_blk, axis=1)
        flat_row = jnp.sum(jnp.where(in_blk, jnp.arange(n_img)[None, :] * block + offset, 0), axis=1)
        flat_row = jnp.where(is_img, flat_row, -1)
        img_mask = is_img[:, None]
        sel = (flat_row[:, None] == jnp.arange(n_img * block)[None, :]).astype(BF)

        pooled_rows = mm(sel, pooled_all).astype(BF)
        normed_rows, norm_pull = jax.vjp(gain_norm, pooled_rows, pn_f)
        flat_all = jnp.where(jnp.any(in_all, axis=1), jnp.sum(jnp.where(in_all, jnp.arange(n_img)[None, :] * block + off_all, 0), axis=1), -1)
        sel_all = (flat_all[:, None] == jnp.arange(n_img * block)[None, :]).astype(BF)
        normed_pos = mm(sel_all, gain_norm(pooled_all, pn_f)).astype(BF)
        soft_rows = mm(normed_rows, w_proj).astype(BF)
        merged = jnp.where(img_mask, soft_rows, text_loc)
        hidden, pre_pull = jax.vjp(gain_norm, merged, pre_f)
        hidden_all = lax.all_gather(hidden, 'cp', tiled=True)

        cos_t, sin_t = rope_tables(pos_all, hd)
        kv_id = rank * kv_heads // size
        wq_h = lax.dynamic_slice(w_query, (0, rank * hd), (dim, hd))
        wk_h = lax.dynamic_slice(w_key, (0, kv_id * hd), (dim, hd))
        wv_h = lax.dynamic_slice(w_value, (0, kv_id * hd), (dim, hd))
        wo_h = lax.dynamic_slice(w_out, (rank * hd, 0), (hd, dim))
        w_head = jnp.concatenate([wq_h, wk_h, wv_h], axis=1)
        q_raw, k_raw, qs, k, kt, v, vt = qkv_call(hidden_all, w_head, cos_t, sin_t, qg_f[None], kg_f[None], bq, scale)

        o, o_wide, lse = attn_fwd(qs, k, vt, lim, lmax, bq, block)
        o_rows = lax.all_to_all(o.reshape(size, loc, hd), 'cp', 0, 0, tiled=True)
        o_rows = o_rows.transpose(1, 0, 2).reshape(loc, heads * hd)
        proj_out = mm(o_rows, w_out).astype(BF)
        y_loc, post_pull = jax.vjp(post_residual, merged, proj_out, post_f)
        d_resid, d_proj, g_post = post_pull(grad_y)

        d_proj_all = lax.all_gather(d_proj, 'cp', tiled=True)
        d_o = mm(d_proj_all, wo_h, ((1,), (1,))).astype(BF)
        g_out_h = mm(o, d_proj_all, ((0,), (0,))).astype(BF)
        d_o, g_out_h = lax.optimization_barrier((d_o, g_out_h))
        g_out = lax.all_gather(g_out_h, 'cp', tiled=True)
        delta = jnp.sum(d_o.astype(F32) * o_wide, axis=1).reshape(nq, 1, bq)
        flag = even.astype(jnp.int32).reshape(1)
        d_q, keep, send = attn_bwd(qs, k, kt, v, d_o, lse, delta, lim, lmax, flag, bq, block, scale)
        got = lax.ppermute(send, 'cp', [(i, i ^ 1) for i in range(size)])
        d_head, g_q_gain, g_k_gain = head_back(flag, d_q, keep, got, q_raw, k_raw, cos_t, sin_t, qg_f[None], kg_f[None], bq)
        g_q_gain, g_k_gain = g_q_gain[0], g_k_gain[0]
        d_rows = lax.all_to_all(d_head.reshape(size, loc, 2 * hd), 'cp', 0, 0, tiled=True)
        g_head = mm(hidden_all, d_head, ((0,), (0,))).astype(BF)
        d_rows, g_head = lax.optimization_barrier((d_rows, g_head))
        g_head_all = lax.all_gather(g_head, 'cp')
        g_query = g_head_all[:, :, :hd].transpose(1, 0, 2).reshape(dim, heads * hd)
        g_key = g_head_all[0::2, :, hd:].transpose(1, 0, 2).reshape(dim, kv_heads * hd)
        g_value = g_head_all[1::2, :, hd:].transpose(1, 0, 2).reshape(dim, kv_heads * hd)

        d_q_flat = d_rows[:, :, :hd].transpose(1, 0, 2).reshape(loc, heads * hd)
        d_k_flat = d_rows[0::2, :, hd:].transpose(1, 0, 2).reshape(loc, kv_heads * hd)
        d_v_flat = d_rows[1::2, :, hd:].transpose(1, 0, 2).reshape(loc, kv_heads * hd)
        nt = ((1,), (1,))
        d_hidden = (mm(d_q_flat, w_query, nt) + mm(d_k_flat, w_key, nt) + mm(d_v_flat, w_value, nt)).astype(BF)
        d_merged_attn, g_pre = pre_pull(d_hidden)
        d_merged = (d_resid.astype(F32) + d_merged_attn.astype(F32)).astype(BF)
        zero = jnp.zeros((), BF)
        grad_text = jnp.where(img_mask, zero, d_merged)
        d_soft = jnp.where(img_mask, d_merged, zero)
        d_normed = mm(d_soft, w_proj, nt).astype(BF)
        d_pooled_rows, g_pn = norm_pull(d_normed)
        d_pooled_all = mm(sel, d_pooled_rows, ((0,), (0,))).astype(BF)
        d_pooled = lax.psum_scatter(d_pooled_all, 'cp', scatter_dimension=0, tiled=True)
        spread = (d_pooled.astype(F32) / (POOL * POOL)).astype(BF)
        grad_vis = mm(pool_mat, spread, ((0,), (0,))).astype(BF)[None]

        cols = dim // size
        d_soft_cols = lax.all_to_all(d_soft.reshape(loc, size, cols).transpose(1, 0, 2), 'cp', 0, 0, tiled=True).reshape(seq, cols)
        g_proj_loc = mm(d_soft_cols, normed_pos, ((0,), (0,))).astype(BF)
        g_proj = lax.all_gather(g_proj_loc, 'cp', tiled=True).T
        small = lax.psum(jnp.concatenate([g_pn, g_pre, g_q_gain, g_k_gain, g_post]), 'cp').astype(BF)
        edges = [0, dim_v, dim_v + dim, dim_v + dim + hd, dim_v + dim + 2 * hd, dim_v + 2 * dim + 2 * hd]
        s_pn, s_pre, s_q, s_k, s_post = (small[a:b] for a, b in zip(edges[:-1], edges[1:]))
        return y_loc, grad_text, grad_vis, s_pn, g_proj, s_pre, g_query, g_key, g_value, s_q, s_k, g_out, s_post

    in_specs = (seq_spec, seq_spec, part_spec, seq_spec) + (rep_spec,) * 10
    out_specs = (seq_spec, seq_spec, seq_spec) + (part_spec,) * 10
    return jax.shard_map(device_body, mesh=mesh, in_specs=in_specs, out_specs=out_specs, check_vma=False)
```
